256 devices in a mesh: gx: 8 (over z), gy: 2 (over core), gz: 16 (over y, x).
Axes of the slice: x: 4, y: 4, z: 8, core: 2. Of those that a mesh axis runs over, the one named last changes fastest.
Arguments:
- pair: bfloat16 [128, 1024, 1024], P('gz', 'gx', 'gy'), may hold values from -6 to 6
- pair_mask: int32 [1024, 1024], P('gx', 'gy'), may hold values from 0 to 1, as said below
- input_gain: float32 [128], replicated, may hold values from 0.1 to 1.9
- input_weights: bfloat16 [4, 128, 128], replicated, may hold values from -0.5 to 0.5
- out_gate_weight: bfloat16 [128, 128], replicated, may hold values from -0.5 to 0.5
- hidden_gain: float32 [128], replicated, may hold values from 0.1 to 1.9
- out_weight: bfloat16 [128, 128], replicated, may hold values from -0.5 to 0.5
Outputs:
- update: bfloat16 [128, 1024, 1024], P('gz', 'gx', 'gy')
The draws below stay inside these ranges and needn't reach their ends.
Inputs may be any that keep to these rules, and one draw needn't show every extreme that they name: pair_mask[r, s] = m[r] * m[s] for a 0/1 residue mask m of the draw that is 0 for all r >= L, for one crop length L with 512 < L <= 1024; residues below L may also be 0.
All inputs are finite; a program needn't handle non-finite values.
Results may differ from the reference program's by a relative error of at most 0.011.
Values may be sent and summed in bfloat16 or wider, within the bound.
A program may use at most 64 MiB of HBM per device.

```python
import jax
import jax.numpy as jnp
from jax import lax

C = 128
CH = 128
N = 1024


def draw_pair_mask(key, part):
    crop_length = jax.random.randint(jax.random.fold_in(key, 7), (), N // 2 + 1, N + 1)
    dropped = jax.random.randint(jax.random.fold_in(key, 11), (N,), 0, 16)
    inside = ((jnp.arange(N) < crop_length) & (dropped != 0)).astype(jnp.int32)
    return inside[:, None] * inside[None, :]


def levels(own_key, extent, split, least, largest):
    loudness, own = 1.0, jax.random.fold_in(own_key, 6)
    for axis_at, shards_of in split:
        steps = jnp.exp(jax.random.uniform(jax.random.fold_in(own, axis_at), (shards_of,), jnp.float32, least / len(split), largest / len(split)))
        loudness = loudness * jnp.repeat(steps, extent[axis_at] // shards_of).reshape([-1 if axis == axis_at else 1 for axis in range(len(extent))])
    return loudness


def bell_draw(stream_key, shape, width, most, cuts=(), kind=jnp.bfloat16):
    factor_of = levels(stream_key, shape, cuts, -0.22, 0.18) if cuts else 1.0
    result = jax.random.normal(stream_key, shape, jnp.float32) * width * factor_of
    return jnp.minimum(jnp.maximum(result, -most), most).astype(kind)


def setup_inputs(seed: int = 0) -> dict:
    seeds = jax.random.split(jax.random.key(seed), 8)
    pair = bell_draw(seeds[0], (C, N, N), 1.0, 6.0, ((0, 16), (1, 8), (2, 2)))
    pair_mask = draw_pair_mask(jax.random.fold_in(seeds[7], 71), 0)
    input_gain = jnp.clip(1.0 + 0.18 * jax.random.normal(seeds[2], (C,), jnp.float32), 0.1, 1.9)
    input_weights = bell_draw(seeds[3], (4, C, CH), C ** -0.5, 0.5)
    out_gate_weight = bell_draw(seeds[4], (C, C), C ** -0.5, 0.5)
    hidden_gain = jnp.clip(1.0 + 0.18 * jax.random.normal(seeds[5], (CH,), jnp.float32), 0.1, 1.9)
    out_weight = bell_draw(seeds[6], (CH, C), CH ** -0.5, 0.5)
    return dict(pair=pair, pair_mask=pair_mask, input_gain=input_gain, input_weights=input_weights, out_gate_weight=out_gate_weight, hidden_gain=hidden_gain, out_weight=out_weight)


EPSILON = 1e-05

def layer_norm(values, gains):
    average = lax.optimization_barrier(jnp.mean(values, axis=0))
    spread = lax.optimization_barrier(jnp.mean(jnp.square(values - average), axis=0))
    return (values - average) * lax.rsqrt(spread + EPSILON) * gains[:, None, None]

def project(weights, normed):
    return jnp.einsum('dk,drs->krs', weights.astype(jnp.float32), normed.astype(jnp.float32))

def reference(pair, pair_mask, input_gain, input_weights, out_gate_weight, hidden_gain, out_weight):
    normed = layer_norm(pair.astype(jnp.float32), input_gain).astype(jnp.bfloat16)
    mask_values = pair_mask.astype(jnp.float32)
    left_side = (mask_values * jax.nn.sigmoid(project(input_weights[0], normed)) * project(input_weights[1], normed)).astype(jnp.bfloat16)
    right_side = (mask_values * jax.nn.sigmoid(project(input_weights[2], normed)) * project(input_weights[3], normed)).astype(jnp.bfloat16)
    gate = jax.nn.sigmoid(project(out_gate_weight, normed))
    triangle = jnp.einsum('hki,hkj->hij', left_side.astype(jnp.float32), right_side.astype(jnp.float32))
    hidden_normed = layer_norm(triangle, hidden_gain).astype(jnp.bfloat16)
    projected = project(out_weight, hidden_normed)
    return (mask_values * gate * projected).astype(jnp.bfloat16)
```

```python
import jax
import jax.numpy as jnp
from jax import lax
from jax.sharding import PartitionSpec as P

EPSILON = 1e-05


def layer_norm(values, gains):
    average = jnp.mean(values, axis=0)
    spread = jnp.mean(jnp.square(values - average), axis=0)
    normed = (values - average) * lax.rsqrt(spread + EPSILON) * gains[:, None, None]
    return normed.astype(jnp.bfloat16)


def exchange(value, axis, split_dim, concat_dim):
    return lax.all_to_all(value, axis, split_axis=split_dim, concat_axis=concat_dim, tiled=True)


def shards(pair, pair_mask, input_gain, input_weights, out_gate_weight, hidden_gain, out_weight):
    channels = input_gain.shape[0]
    hidden = hidden_gain.shape[0]
    rows = pair.shape[1] // lax.axis_size("gz")
    share_mask = lax.dynamic_slice_in_dim(
        pair_mask, lax.axis_index("gz") * rows, rows, 0
    ).astype(jnp.float32)

    normed = layer_norm(exchange(pair, "gz", 1, 0).astype(jnp.float32), input_gain)
    weights = jnp.concatenate([*input_weights, out_gate_weight], axis=1)
    product = jnp.einsum("dk,drs->krs", weights, normed, preferred_element_type=jnp.float32)
    left_gate, left, right_gate, right = (product[k * hidden : (k + 1) * hidden] for k in range(4))
    gate = share_mask * jax.nn.sigmoid(product[4 * hidden :])
    sides = jnp.stack(
        [
            (share_mask * jax.nn.sigmoid(left_gate) * left).astype(jnp.bfloat16),
            (share_mask * jax.nn.sigmoid(right_gate) * right).astype(jnp.bfloat16),
        ],
        axis=1,
    )

    sides = exchange(sides, "gz", 0, 2)
    sides = exchange(sides, "gx", 0, 2)
    left_side = lax.all_gather(sides[:, 0], "gy", axis=2, tiled=True)
    triangle = jnp.einsum(
        "hki,hkj->hij", left_side, sides[:, 1], preferred_element_type=jnp.float32
    ).astype(jnp.bfloat16)
    triangle = exchange(triangle, "gx", 1, 0)
    triangle = exchange(triangle, "gz", 1, 0)

    hidden_normed = layer_norm(triangle.astype(jnp.float32), hidden_gain)
    projected = jnp.einsum(
        "hc,hij->cij", out_weight, hidden_normed, preferred_element_type=jnp.float32
    )
    update = (gate * projected).astype(jnp.bfloat16)
    return exchange(update, "gz", 0, 1)


def solution(mesh):
    placed = (P("gz", "gx", "gy"), P("gx", "gy"), P(), P(), P(), P(), P())
    return jax.shard_map(
        shards, mesh=mesh, in_specs=placed, out_specs=P("gz", "gx", "gy"), check_vma=False
    )
```

```python
import functools

import jax
import jax.numpy as jnp
from jax import lax
from jax.experimental import pallas as pl
from jax.experimental.pallas import tpu as pltpu
from jax.sharding import PartitionSpec as P

EPSILON = 1e-05
MESH = pl.DeviceIdType.MESH
PARTS = 2
LANES = 128


def statistics(values):
    average = jnp.mean(values, axis=0)
    centred = values - average
    return centred * lax.rsqrt(jnp.mean(jnp.square(centred), axis=0) + EPSILON)


def kernel(
    nx, ng,
    pair, mask, input_gain, input_weights, gate_weight, hidden_gain, out_weight,
    out,
    shared, sides, left_right, other_left, turned, triangle, hidden, update, gate,
    weights, gains, rows_in, rows_left, rows_right,
    send, got_shared, got_sides, got_left, got_hidden, got_out,
):
    x, y, g = lax.axis_index("gx"), lax.axis_index("gy"), lax.axis_index("gz")
    chips = nx * ng
    me = x * ng + g
    depth = pair.shape[0]
    rows = pair.shape[1] // ng
    width = pair.shape[2] // PARTS
    channels = gate_weight.shape[0]
    long = turned.shape[0]

    def device(chip):
        return (chip // ng, y, lax.rem(chip, ng))

    barrier = pltpu.get_barrier_semaphore()

    @pl.loop(1, chips)
    def _(step):
        pl.semaphore_signal(
            barrier, inc=1, device_id=device(lax.rem(me + step, chips)), device_id_type=MESH
        )

    pl.semaphore_signal(barrier, inc=1, device_id=(x, 1 - y, g), device_id_type=MESH)

    for k in range(4):
        weights[k * channels : (k + 1) * channels] = (
            input_weights[k].astype(jnp.float32).T.astype(jnp.bfloat16)
        )
    weights[4 * channels : 5 * channels] = gate_weight[...].astype(jnp.float32).T.astype(jnp.bfloat16)
    weights[5 * channels :] = out_weight[...].astype(jnp.float32).T.astype(jnp.bfloat16)
    gains[0] = jnp.broadcast_to(input_gain[...], (channels, channels)).T
    gains[1] = jnp.broadcast_to(hidden_gain[...], (channels, channels)).T

    pl.semaphore_wait(barrier, chips)

    my_rows = pl.ds(pl.multiple_of(g * rows, rows), rows)
    my_channels = pl.ds(pl.multiple_of(g * depth, depth), depth)
    for q in range(PARTS):
        columns = pl.ds(q * width, width)

        @pl.loop(1, ng)
        def _(step):
            peer = lax.rem(g + step, ng)
            pltpu.make_async_remote_copy(
                src_ref=pair.at[:, pl.ds(pl.multiple_of(peer * rows, rows), rows), columns],
                dst_ref=shared.at[q, my_channels],
                send_sem=send.at[0],
                recv_sem=got_shared.at[q],
                device_id=(x, y, peer),
                device_id_type=MESH,
            ).start()

        pltpu.make_async_copy(
            pair.at[:, my_rows, columns], shared.at[q, my_channels], got_shared.at[q]
        ).start()

    stride = rows
    block = pl.ds(pl.multiple_of(me * rows, rows), rows)
    for q in range(PARTS):
        pltpu.make_async_copy(shared.at[q], shared.at[q], got_shared.at[q]).wait()
        for at in range(width // LANES):
            lanes = pl.ds(at * LANES, LANES)
            normed = statistics(shared[q, :, :, lanes].astype(jnp.float32))
            rows_in[pl.ds(0, channels * rows)] = normed.reshape(channels * rows, LANES)
            share_mask = mask[my_rows, pl.ds(q * width + at * LANES, LANES)].astype(jnp.float32)
            rows_in[pl.ds(channels * rows, rows)] = share_mask

            @pl.loop(0, rows)
            def _(r):
                take = pl.ds(r, channels, stride=stride)
                one = (rows_in[take, :] * gains[0]).astype(jnp.bfloat16)
                product = jnp.dot(
                    weights[: 5 * channels], one, preferred_element_type=jnp.float32
                )
                keep = rows_in[pl.ds(channels * rows + r, 1), :]
                a, b, c, d, e = (product[k * channels : (k + 1) * channels] for k in range(5))
                rows_left[take, :] = keep * jax.nn.sigmoid(a) * b
                rows_right[take, :] = keep * jax.nn.sigmoid(c) * d
                gate[q * (width // LANES) + at, r] = keep * jax.nn.sigmoid(e)

            sides[q, :, 0, :, lanes] = (
                rows_left[...].reshape(channels, rows, LANES).astype(jnp.bfloat16)
            )
            sides[q, :, 1, :, lanes] = (
                rows_right[...].reshape(channels, rows, LANES).astype(jnp.bfloat16)
            )

        @pl.loop(1, chips)
        def _(step):
            owner = lax.rem(me + step, chips)
            pltpu.make_async_remote_copy(
                src_ref=sides.at[q, owner],
                dst_ref=left_right.at[q, :, block, :],
                send_sem=send.at[1],
                recv_sem=got_sides.at[q],
                device_id=device(owner),
                device_id_type=MESH,
            ).start()

        pltpu.make_async_copy(
            sides.at[q, me], left_right.at[q, :, block, :], got_sides.at[q]
        ).start()

    half = PARTS * width
    for q in range(PARTS):
        pltpu.make_async_copy(left_right.at[q], left_right.at[q], got_sides.at[q]).wait()
        pltpu.make_async_remote_copy(
            src_ref=left_right.at[q, 0],
            dst_ref=other_left.at[q],
            send_sem=send.at[2],
            recv_sem=got_left.at[q],
            device_id=(x, 1 - y, g),
            device_id_type=MESH,
        ).start()
        for at in range(width // LANES):
            turned[pl.ds(pl.multiple_of(y * half + q * width + at * LANES, LANES), LANES), :] = (
                left_right[q, 0, :, pl.ds(at * LANES, LANES)].T
            )
    for q in range(PARTS):
        pltpu.make_async_copy(other_left.at[q], other_left.at[q], got_left.at[q]).wait()
        for at in range(width // LANES):
            turned[
                pl.ds(pl.multiple_of((1 - y) * half + q * width + at * LANES, LANES), LANES), :
            ] = other_left[q, :, pl.ds(at * LANES, LANES)].T

    tall = rows * ng
    for q in range(PARTS):

        @pl.loop(0, nx)
        def _(step):
            plane = lax.rem(x + step, nx)
            some = pl.ds(pl.multiple_of(plane * tall, tall), tall)
            triangle[q, some, :] = jnp.dot(
                turned[some, :], left_right[q, 1], preferred_element_type=jnp.float32
            ).astype(jnp.bfloat16)

        @pl.loop(1, chips)
        def _(step):
            owner = lax.rem(me + step, chips)
            pltpu.make_async_remote_copy(
                src_ref=triangle.at[q, pl.ds(pl.multiple_of(owner * rows, rows), rows), :],
                dst_ref=hidden.at[q, me],
                send_sem=send.at[3],
                recv_sem=got_hidden.at[q],
                device_id=device(owner),
                device_id_type=MESH,
            ).start()

        pltpu.make_async_copy(
            triangle.at[q, block, :], hidden.at[q, me], got_hidden.at[q]
        ).start()

    for q in range(PARTS):
        columns = pl.ds(q * width, width)
        pltpu.make_async_copy(hidden.at[q], hidden.at[q], got_hidden.at[q]).wait()
        for at in range(width // LANES):
            lanes = pl.ds(at * LANES, LANES)
            normed = statistics(hidden[q, :, :, lanes].astype(jnp.float32))
            rows_in[pl.ds(0, channels * rows)] = normed.reshape(channels * rows, LANES)

            @pl.loop(0, rows)
            def _(r):
                take = pl.ds(r, channels, stride=stride)
                one = (rows_in[take, :] * gains[1]).astype(jnp.bfloat16)
                projected = jnp.dot(
                    weights[5 * channels :], one, preferred_element_type=jnp.float32
                )
                rows_left[take, :] = gate[q * (width // LANES) + at, r] * projected

            update[q, :, :, lanes] = (
                rows_left[...].reshape(channels, rows, LANES).astype(jnp.bfloat16)
            )

        @pl.loop(1, ng)
        def _(step):
            peer = lax.rem(g + step, ng)
            pltpu.make_async_remote_copy(
                src_ref=update.at[q, pl.ds(pl.multiple_of(peer * depth, depth), depth)],
                dst_ref=out.at[:, my_rows, columns],
                send_sem=send.at[4],
                recv_sem=got_out,
                device_id=(x, y, peer),
                device_id_type=MESH,
            ).start()

        pltpu.make_async_copy(update.at[q, my_channels], out.at[:, my_rows, columns], got_out).start()

    pltpu.make_async_copy(out, out, got_out).wait()
    for q in range(PARTS):
        few = shared.at[q, pl.ds(0, (ng - 1) * depth)]
        pltpu.make_async_copy(few, few, send.at[0]).wait()
        most = sides.at[q, pl.ds(0, chips - 1)]
        pltpu.make_async_copy(most, most, send.at[1]).wait()
        pltpu.make_async_copy(other_left.at[q], other_left.at[q], send.at[2]).wait()
        most = triangle.at[q, pl.ds(0, (chips - 1) * rows)]
        pltpu.make_async_copy(most, most, send.at[3]).wait()
        few = update.at[q, pl.ds(0, (ng - 1) * depth)]
        pltpu.make_async_copy(few, few, send.at[4]).wait()


def shards(mesh, pair, pair_mask, input_gain, input_weights, out_gate_weight, hidden_gain, out_weight):
    nx, ng = mesh.shape["gx"], mesh.shape["gz"]
    chips = nx * ng
    channels, hidden = input_weights.shape[1:]
    depth, tall, wide = pair.shape
    rows, width, long = tall // ng, wide // PARTS, tall * nx
    low, full = jnp.bfloat16, jnp.float32
    vmem = pl.BlockSpec(memory_space=pltpu.VMEM)
    return pl.pallas_call(
        functools.partial(kernel, nx, ng),
        out_shape=jax.ShapeDtypeStruct(pair.shape, low),
        in_specs=[vmem] * 7,
        out_specs=vmem,
        scratch_shapes=[
            pltpu.VMEM((PARTS, channels, rows, width), low),
            pltpu.VMEM((PARTS, hidden, 2, rows, width), low),
            pltpu.VMEM((PARTS, 2, long, width), low),
            pltpu.VMEM((PARTS, long, width), low),
            pltpu.VMEM((2 * wide, long), low),
            pltpu.VMEM((PARTS, long, width), low),
            pltpu.VMEM((PARTS, hidden, rows, width), low),
            pltpu.VMEM((PARTS, channels, rows, width), low),
            pltpu.VMEM((wide // LANES, rows, channels, LANES), full),
            pltpu.VMEM((6 * channels, channels), low),
            pltpu.VMEM((2, channels, channels), full),
            pltpu.VMEM((channels * rows + rows, LANES), full),
            pltpu.VMEM((channels * rows, LANES), full),
            pltpu.VMEM((channels * rows, LANES), full),
            pltpu.SemaphoreType.DMA((5,)),
            pltpu.SemaphoreType.DMA((PARTS,)),
            pltpu.SemaphoreType.DMA((PARTS,)),
            pltpu.SemaphoreType.DMA((PARTS,)),
            pltpu.SemaphoreType.DMA((PARTS,)),
            pltpu.SemaphoreType.DMA(()),
        ],
        compiler_params=pltpu.CompilerParams(collective_id=0, has_side_effects=True),
    )(
        pair, pair_mask, input_gain[None], input_weights, out_gate_weight, hidden_gain[None], out_weight
    )


def solution(mesh):
    placed = (P("gz", "gx", "gy"), P("gx", "gy"), P(), P(), P(), P(), P())
    return jax.shard_map(
        functools.partial(shards, mesh),
        mesh=mesh,
        in_specs=placed,
        out_specs=P("gz", "gx", "gy"),
        check_vma=False,
    )
```

```python
import functools

import jax
import jax.numpy as jnp
from jax import lax
from jax.experimental import pallas as pl
from jax.experimental.pallas import tpu as pltpu
from jax.sharding import PartitionSpec as P

EPSILON = 1e-05
MESH = pl.DeviceIdType.MESH
LANES = 128
PARTS = 4


def statistics(values):
    average = jnp.mean(values, axis=0)
    centred = values - average
    return centred * lax.rsqrt(jnp.mean(jnp.square(centred), axis=0) + EPSILON)


def kernel(
    nx, ng,
    pair_in, mask_in, input_gain, input_weights_in, gate_weight_in, hidden_gain, out_weight_in,
    out,
    pair, mask, input_weights, gate_weight, out_weight,
    shared, ones, left, right, all_left, all_right, other_left, turned, triangle, hidden, update, gate,
    weights, gains, rows_in, rows_out, rows_kept,
    loaded, send, got_shared, got_left, got_right, got_other, got_hidden, got_out, planes,
):
    x, y, g = lax.axis_index("gx"), lax.axis_index("gy"), lax.axis_index("gz")
    chips = nx * ng
    me = x * ng + g
    depth = pair.shape[0]
    rows = pair.shape[1] // ng
    channels = gate_weight.shape[0]
    wide = PARTS * LANES
    tall = ng * rows

    def plane_at(step):
        far = (step + 1) // 2
        return lax.rem(x + lax.rem(step, 2) * far + (1 - lax.rem(step, 2)) * (nx - far), nx)

    def aligned(at, size):
        return pl.ds(pl.multiple_of(at * size, size), size)

    barrier = pltpu.get_barrier_semaphore()

    @pl.loop(1, ng)
    def _(step):
        pl.semaphore_signal(
            barrier, inc=1, device_id=(x, y, lax.rem(g + step, ng)), device_id_type=MESH
        )

    @pl.loop(1, nx)
    def _(step):
        pl.semaphore_signal(barrier, inc=1, device_id=(plane_at(step), y, g), device_id_type=MESH)

    pl.semaphore_signal(barrier, inc=1, device_id=(x, 1 - y, g), device_id_type=MESH)

    loads = [
        pltpu.make_async_copy(there, here, loaded.at[k])
        for k, (there, here) in enumerate(
            (
                (pair_in, pair),
                (input_weights_in, input_weights),
                (gate_weight_in, gate_weight),
                (out_weight_in, out_weight),
                (mask_in, mask),
            )
        )
    ]
    for load in loads:
        load.start()
    gains[0] = jnp.broadcast_to(input_gain[...], (channels, channels)).T
    gains[1] = jnp.broadcast_to(hidden_gain[...], (channels, channels)).T
    for load in loads:
        load.wait()

    pl.semaphore_wait(barrier, ng + nx - 1)

    my_rows = aligned(g, rows)
    my_channels = aligned(g, depth)
    for q in range(PARTS):
        columns = pl.ds(q * LANES, LANES)

        @pl.loop(1, ng)
        def _(step):
            peer = lax.rem(g + step, ng)
            pltpu.make_async_remote_copy(
                src_ref=pair.at[:, aligned(peer, rows), columns],
                dst_ref=shared.at[q, my_channels],
                send_sem=send.at[0],
                recv_sem=got_shared.at[q],
                device_id=(x, y, peer),
                device_id_type=MESH,
            ).start()

        pltpu.make_async_copy(
            pair.at[:, my_rows, columns], shared.at[q, my_channels], got_shared.at[q]
        ).start()

    @pl.loop(1, nx)
    def _(step):
        pl.semaphore_signal(planes, inc=1, device_id=(plane_at(step), y, g), device_id_type=MESH)

    for k in range(4):
        weights[k * channels : (k + 1) * channels] = (
            input_weights[k].astype(jnp.float32).T.astype(jnp.bfloat16)
        )
    weights[4 * channels : 5 * channels] = gate_weight[...].astype(jnp.float32).T.astype(jnp.bfloat16)
    weights[5 * channels :] = out_weight[...].astype(jnp.float32).T.astype(jnp.bfloat16)

    block = aligned(me, rows)

    def to_owners(side, whole, got, q):
        @pl.loop(1, chips)
        def _(step):
            plane, column = plane_at(lax.rem(step, nx)), lax.rem(g + step // nx, ng)
            pltpu.make_async_remote_copy(
                src_ref=side.at[q, plane * ng + column],
                dst_ref=whole.at[q, block, :],
                send_sem=send.at[1],
                recv_sem=got.at[q],
                device_id=(plane, y, column),
                device_id_type=MESH,
            ).start()

        pltpu.make_async_copy(side.at[q, me], whole.at[q, block, :], got.at[q]).start()

    for q in range(PARTS):
        pltpu.make_async_copy(shared.at[q], shared.at[q], got_shared.at[q]).wait()
        normed = statistics(shared[q].astype(jnp.float32))
        rows_in[...] = normed.reshape(channels * rows, LANES)
        rows_kept[q] = mask[my_rows, pl.ds(q * LANES, LANES)].astype(jnp.float32)

        @pl.loop(0, rows)
        def _(r):
            take = pl.ds(r, channels, stride=rows)
            one = (rows_in[take, :] * gains[0]).astype(jnp.bfloat16)
            ones[q, r] = one
            product = jnp.dot(weights[: 2 * channels], one, preferred_element_type=jnp.float32)
            rows_out[take, :] = (
                rows_kept[q, pl.ds(r, 1), :]
                * jax.nn.sigmoid(product[:channels])
                * product[channels:]
            )

        left[q] = rows_out[...].reshape(channels, rows, LANES).astype(jnp.bfloat16)
        if q == 0:
            pl.semaphore_wait(planes, nx - 1)
        to_owners(left, all_left, got_left, q)

    for q in range(PARTS):

        @pl.loop(0, rows)
        def _(r):
            product = jnp.dot(
                weights[2 * channels : 5 * channels], ones[q, r], preferred_element_type=jnp.float32
            )
            keep = rows_kept[q, pl.ds(r, 1), :]
            rows_out[pl.ds(r, channels, stride=rows), :] = (
                keep * jax.nn.sigmoid(product[:channels]) * product[channels : 2 * channels]
            )
            gate[q, r] = keep * jax.nn.sigmoid(product[2 * channels :])

        right[q] = rows_out[...].reshape(channels, rows, LANES).astype(jnp.bfloat16)
        to_owners(right, all_right, got_right, q)

    for q in range(PARTS):
        pltpu.make_async_copy(all_left.at[q], all_left.at[q], got_left.at[q]).wait()
        pltpu.make_async_remote_copy(
            src_ref=all_left.at[q],
            dst_ref=other_left.at[q],
            send_sem=send.at[2],
            recv_sem=got_other.at[q],
            device_id=(x, 1 - y, g),
            device_id_type=MESH,
        ).start()
        turned[aligned(y * PARTS + q, LANES), :] = all_left[q].T
    for q in range(PARTS):
        pltpu.make_async_copy(other_left.at[q], other_left.at[q], got_other.at[q]).wait()
        turned[aligned((1 - y) * PARTS + q, LANES), :] = other_left[q].T

    for q in range(PARTS):
        pltpu.make_async_copy(all_right.at[q], all_right.at[q], got_right.at[q]).wait()

        @pl.loop(0, nx)
        def _(step):
            plane = plane_at(nx - 1 - step)
            some = aligned(plane, tall)
            triangle[q, some, :] = jnp.dot(
                turned[some, :], all_right[q], preferred_element_type=jnp.float32
            ).astype(jnp.bfloat16)

            @pl.loop(0, ng)
            def _(turn):
                column = lax.rem(g + turn, ng)

                @pl.when((step != nx - 1) | (turn != 0))
                def _():
                    pltpu.make_async_remote_copy(
                        src_ref=triangle.at[q, aligned(plane * ng + column, rows), :],
                        dst_ref=hidden.at[q, me],
                        send_sem=send.at[3],
                        recv_sem=got_hidden.at[q],
                        device_id=(plane, y, column),
                        device_id_type=MESH,
                    ).start()

        pltpu.make_async_copy(
            triangle.at[q, block, :], hidden.at[q, me], got_hidden.at[q]
        ).start()

    for q in range(PARTS):
        columns = pl.ds(q * LANES, LANES)
        pltpu.make_async_copy(hidden.at[q], hidden.at[q], got_hidden.at[q]).wait()
        normed = statistics(hidden[q].astype(jnp.float32))
        rows_in[...] = normed.reshape(channels * rows, LANES)

        @pl.loop(0, rows)
        def _(r):
            take = pl.ds(r, channels, stride=rows)
            one = (rows_in[take, :] * gains[1]).astype(jnp.bfloat16)
            projected = jnp.dot(weights[5 * channels :], one, preferred_element_type=jnp.float32)
            rows_out[take, :] = gate[q, r] * projected

        update[q] = rows_out[...].reshape(channels, rows, LANES).astype(jnp.bfloat16)

        @pl.loop(1, ng)
        def _(step):
            peer = lax.rem(g + step, ng)
            pltpu.make_async_remote_copy(
                src_ref=update.at[q, aligned(peer, depth)],
                dst_ref=out.at[:, my_rows, columns],
                send_sem=send.at[4],
                recv_sem=got_out,
                device_id=(x, y, peer),
                device_id_type=MESH,
            ).start()

        pltpu.make_async_copy(update.at[q, my_channels], out.at[:, my_rows, columns], got_out).start()

    pltpu.make_async_copy(out, out, got_out).wait()
    for q in range(PARTS):
        few = shared.at[q, pl.ds(0, (ng - 1) * depth)]
        pltpu.make_async_copy(few, few, send.at[0]).wait()
        for side in (left, right):
            most = side.at[q, pl.ds(0, chips - 1)]
            pltpu.make_async_copy(most, most, send.at[1]).wait()
        pltpu.make_async_copy(other_left.at[q], other_left.at[q], send.at[2]).wait()
        most = triangle.at[q, pl.ds(0, (chips - 1) * rows)]
        pltpu.make_async_copy(most, most, send.at[3]).wait()
        few = update.at[q, pl.ds(0, (ng - 1) * depth)]
        pltpu.make_async_copy(few, few, send.at[4]).wait()


def shards(mesh, pair, pair_mask, input_gain, input_weights, out_gate_weight, hidden_gain, out_weight):
    nx, ng = mesh.shape["gx"], mesh.shape["gz"]
    channels, hidden = input_weights.shape[1:]
    rows, long = pair.shape[1] // ng, pair.shape[1] * nx
    low, full = jnp.bfloat16, jnp.float32
    vmem, where = pl.BlockSpec(memory_space=pltpu.VMEM), pl.BlockSpec(memory_space=pl.ANY)
    parts = pltpu.SemaphoreType.DMA((PARTS,))
    return pl.pallas_call(
        functools.partial(kernel, nx, ng),
        out_shape=jax.ShapeDtypeStruct(pair.shape, low),
        in_specs=[where, where, vmem, where, where, vmem, where],
        out_specs=where,
        scratch_shapes=[
            pltpu.VMEM(pair.shape, low),
            pltpu.VMEM(pair_mask.shape, jnp.int32),
            pltpu.VMEM(input_weights.shape, low),
            pltpu.VMEM(out_gate_weight.shape, low),
            pltpu.VMEM(out_weight.shape, low),
            pltpu.VMEM((PARTS, channels, rows, LANES), low),
            pltpu.VMEM((PARTS, rows, channels, LANES), low),
            pltpu.VMEM((PARTS, hidden, rows, LANES), low),
            pltpu.VMEM((PARTS, hidden, rows, LANES), low),
            pltpu.VMEM((PARTS, long, LANES), low),
            pltpu.VMEM((PARTS, long, LANES), low),
            pltpu.VMEM((PARTS, long, LANES), low),
            pltpu.VMEM((2 * PARTS * LANES, long), low),
            pltpu.VMEM((PARTS, long, LANES), low),
            pltpu.VMEM((PARTS, hidden, rows, LANES), low),
            pltpu.VMEM((PARTS, channels, rows, LANES), low),
            pltpu.VMEM((PARTS, rows, channels, LANES), full),
            pltpu.VMEM((6 * channels, channels), low),
            pltpu.VMEM((2, channels, channels), full),
            pltpu.VMEM((channels * rows, LANES), full),
            pltpu.VMEM((channels * rows, LANES), full),
            pltpu.VMEM((PARTS, rows, LANES), full),
            pltpu.SemaphoreType.DMA((5,)),
            pltpu.SemaphoreType.DMA((5,)),
            parts,
            parts,
            parts,
            parts,
            parts,
            pltpu.SemaphoreType.DMA(()),
            pltpu.SemaphoreType.REGULAR,
        ],
        compiler_params=pltpu.CompilerParams(collective_id=0, has_side_effects=True),
    )(
        pair, pair_mask, input_gain[None], input_weights, out_gate_weight, hidden_gain[None], out_weight
    )


def solution(mesh):
    placed = (P("gz", "gx", "gy"), P("gx", "gy"), P(), P(), P(), P(), P())
    return jax.shard_map(
        functools.partial(shards, mesh),
        mesh=mesh,
        in_specs=placed,
        out_specs=P("gz", "gx", "gy"),
        check_vma=False,
    )
```

```python
import functools

import jax
import jax.numpy as jnp
from jax import lax
from jax.experimental import pallas as pl
from jax.experimental.pallas import tpu as pltpu
from jax.sharding import PartitionSpec as P

EPSILON = 1e-05
MESH = pl.DeviceIdType.MESH
LANES = 128
PARTS = 4


def statistics(values):
    average = jnp.mean(values, axis=0)
    centred = values - average
    return centred * lax.rsqrt(jnp.mean(jnp.square(centred), axis=0) + EPSILON)


def kernel(
    nx, ng,
    pair_in, mask_in, input_gain, input_weights_in, gate_weight_in, hidden_gain, out_weight_in,
    out,
    pair, mask, input_weights, gate_weight, out_weight,
    shared, ones, left, right, all_left, all_right, other_left, turned, triangle, hidden, update, gate,
    weights, gains, rows_in, rows_out, rows_kept,
    loaded, send, got_shared, got_left, got_right, got_other, got_hidden, got_out, planes,
):
    x, y, g = lax.axis_index("gx"), lax.axis_index("gy"), lax.axis_index("gz")
    chips = nx * ng
    me = x * ng + g
    depth = pair.shape[0]
    rows = pair.shape[1] // ng
    channels = gate_weight.shape[0]
    wide = PARTS * LANES
    tall = ng * rows

    def plane_at(step):
        far = (step + 1) // 2
        return lax.rem(x + lax.rem(step, 2) * far + (1 - lax.rem(step, 2)) * (nx - far), nx)

    def aligned(at, size):
        return pl.ds(pl.multiple_of(at * size, size), size)

    barrier = pltpu.get_barrier_semaphore()

    @pl.loop(1, ng)
    def _(step):
        pl.semaphore_signal(
            barrier, inc=1, device_id=(x, y, lax.rem(g + step, ng)), device_id_type=MESH
        )

    @pl.loop(1, nx)
    def _(step):
        pl.semaphore_signal(barrier, inc=1, device_id=(plane_at(step), y, g), device_id_type=MESH)

    pl.semaphore_signal(barrier, inc=1, device_id=(x, 1 - y, g), device_id_type=MESH)

    loads = [
        pltpu.make_async_copy(there, here, loaded.at[k])
        for k, (there, here) in enumerate(
            (
                (pair_in, pair),
                (input_weights_in, input_weights),
                (gate_weight_in, gate_weight),
                (out_weight_in, out_weight),
                (mask_in, mask),
            )
        )
    ]
    for load in loads:
        load.start()
    gains[0] = jnp.broadcast_to(input_gain[...], (channels, channels)).T
    gains[1] = jnp.broadcast_to(hidden_gain[...], (channels, channels)).T
    for load in loads:
        load.wait()

    pl.semaphore_wait(barrier, ng + nx - 1)

    my_rows = aligned(g, rows)
    my_channels = aligned(g, depth)
    for q in range(PARTS):
        columns = pl.ds(q * LANES, LANES)

        @pl.loop(1, ng)
        def _(step):
            peer = lax.rem(g + step, ng)
            pltpu.make_async_remote_copy(
                src_ref=pair.at[:, aligned(peer, rows), columns],
                dst_ref=shared.at[q, my_channels],
                send_sem=send.at[0],
                recv_sem=got_shared.at[q],
                device_id=(x, y, peer),
                device_id_type=MESH,
            ).start()

        pltpu.make_async_copy(
            pair.at[:, my_rows, columns], shared.at[q, my_channels], got_shared.at[q]
        ).start()

    @pl.loop(1, nx)
    def _(step):
        pl.semaphore_signal(planes, inc=1, device_id=(plane_at(step), y, g), device_id_type=MESH)

    for k in range(4):
        weights[k * channels : (k + 1) * channels] = (
            input_weights[k].astype(jnp.float32).T.astype(jnp.bfloat16)
        )
    weights[4 * channels : 5 * channels] = gate_weight[...].astype(jnp.float32).T.astype(jnp.bfloat16)
    weights[5 * channels :] = out_weight[...].astype(jnp.float32).T.astype(jnp.bfloat16)

    block = aligned(me, rows)

    def to_owners(side, whole, got, q):
        @pl.loop(1, chips)
        def _(step):
            plane, column = plane_at(lax.rem(step, nx)), lax.rem(g + step // nx, ng)
            pltpu.make_async_remote_copy(
                src_ref=side.at[q, plane * ng + column],
                dst_ref=whole.at[q, block, :],
                send_sem=send.at[1],
                recv_sem=got.at[q],
                device_id=(plane, y, column),
                device_id_type=MESH,
            ).start()

        pltpu.make_async_copy(side.at[q, me], whole.at[q, block, :], got.at[q]).start()

    for q in range(PARTS):
        pltpu.make_async_copy(shared.at[q], shared.at[q], got_shared.at[q]).wait()
        normed = statistics(shared[q].astype(jnp.float32))
        rows_in[...] = normed.reshape(channels * rows, LANES)
        rows_kept[q] = mask[my_rows, pl.ds(q * LANES, LANES)].astype(jnp.float32)

        @pl.loop(0, rows, unroll=8)
        def _(r):
            take = pl.ds(r, channels, stride=rows)
            one = (rows_in[take, :] * gains[0]).astype(jnp.bfloat16)
            ones[q, r] = one
            product = jnp.dot(weights[: 2 * channels], one, preferred_element_type=jnp.float32)
            rows_out[take, :] = (
                rows_kept[q, pl.ds(r, 1), :]
                * jax.nn.sigmoid(product[:channels])
                * product[channels:]
            )

        left[q] = rows_out[...].reshape(channels, rows, LANES).astype(jnp.bfloat16)
        if q == 0:
            pl.semaphore_wait(planes, nx - 1)
        to_owners(left, all_left, got_left, q)

    for q in range(PARTS):

        @pl.loop(0, rows, unroll=8)
        def _(r):
            product = jnp.dot(
                weights[2 * channels : 5 * channels], ones[q, r], preferred_element_type=jnp.float32
            )
            keep = rows_kept[q, pl.ds(r, 1), :]
            rows_out[pl.ds(r, channels, stride=rows), :] = (
                keep * jax.nn.sigmoid(product[:channels]) * product[channels : 2 * channels]
            )
            gate[q, r] = keep * jax.nn.sigmoid(product[2 * channels :])

        right[q] = rows_out[...].reshape(channels, rows, LANES).astype(jnp.bfloat16)
        to_owners(right, all_right, got_right, q)

    for q in range(PARTS):
        pltpu.make_async_copy(all_left.at[q], all_left.at[q], got_left.at[q]).wait()
        pltpu.make_async_remote_copy(
            src_ref=all_left.at[q],
            dst_ref=other_left.at[q],
            send_sem=send.at[2],
            recv_sem=got_other.at[q],
            device_id=(x, 1 - y, g),
            device_id_type=MESH,
        ).start()
        turned[aligned(y * PARTS + q, LANES), :] = all_left[q].T
    for q in range(PARTS):
        pltpu.make_async_copy(other_left.at[q], other_left.at[q], got_other.at[q]).wait()
        turned[aligned((1 - y) * PARTS + q, LANES), :] = other_left[q].T

    for q in range(PARTS):
        pltpu.make_async_copy(all_right.at[q], all_right.at[q], got_right.at[q]).wait()

        @pl.loop(0, nx)
        def _(step):
            plane = plane_at(nx - 1 - step)
            some = aligned(plane, tall)
            triangle[q, some, :] = jnp.dot(
                turned[some, :], all_right[q], preferred_element_type=jnp.float32
            ).astype(jnp.bfloat16)

            @pl.loop(0, ng)
            def _(turn):
                column = lax.rem(g + turn, ng)

                @pl.when((step != nx - 1) | (turn != 0))
                def _():
                    pltpu.make_async_remote_copy(
                        src_ref=triangle.at[q, aligned(plane * ng + column, rows), :],
                        dst_ref=hidden.at[q, me],
                        send_sem=send.at[3],
                        recv_sem=got_hidden.at[q],
                        device_id=(plane, y, column),
                        device_id_type=MESH,
                    ).start()

        pltpu.make_async_copy(
            triangle.at[q, block, :], hidden.at[q, me], got_hidden.at[q]
        ).start()

    for q in range(PARTS):
        columns = pl.ds(q * LANES, LANES)
        pltpu.make_async_copy(hidden.at[q], hidden.at[q], got_hidden.at[q]).wait()
        normed = statistics(hidden[q].astype(jnp.float32))
        rows_in[...] = normed.reshape(channels * rows, LANES)

        @pl.loop(0, rows, unroll=8)
        def _(r):
            take = pl.ds(r, channels, stride=rows)
            one = (rows_in[take, :] * gains[1]).astype(jnp.bfloat16)
            projected = jnp.dot(weights[5 * channels :], one, preferred_element_type=jnp.float32)
            rows_out[take, :] = gate[q, r] * projected

        update[q] = rows_out[...].reshape(channels, rows, LANES).astype(jnp.bfloat16)

        @pl.loop(1, ng)
        def _(step):
            peer = lax.rem(g + step, ng)
            pltpu.make_async_remote_copy(
                src_ref=update.at[q, aligned(peer, depth)],
                dst_ref=out.at[:, my_rows, columns],
                send_sem=send.at[4],
                recv_sem=got_out,
                device_id=(x, y, peer),
                device_id_type=MESH,
            ).start()

        pltpu.make_async_copy(update.at[q, my_channels], out.at[:, my_rows, columns], got_out).start()

    pltpu.make_async_copy(out, out, got_out).wait()
    for q in range(PARTS):
        few = shared.at[q, pl.ds(0, (ng - 1) * depth)]
        pltpu.make_async_copy(few, few, send.at[0]).wait()
        for side in (left, right):
            most = side.at[q, pl.ds(0, chips - 1)]
            pltpu.make_async_copy(most, most, send.at[1]).wait()
        pltpu.make_async_copy(other_left.at[q], other_left.at[q], send.at[2]).wait()
        most = triangle.at[q, pl.ds(0, (chips - 1) * rows)]
        pltpu.make_async_copy(most, most, send.at[3]).wait()
        few = update.at[q, pl.ds(0, (ng - 1) * depth)]
        pltpu.make_async_copy(few, few, send.at[4]).wait()


def shards(mesh, pair, pair_mask, input_gain, input_weights, out_gate_weight, hidden_gain, out_weight):
    nx, ng = mesh.shape["gx"], mesh.shape["gz"]
    channels, hidden = input_weights.shape[1:]
    rows, long = pair.shape[1] // ng, pair.shape[1] * nx
    low, full = jnp.bfloat16, jnp.float32
    vmem, where = pl.BlockSpec(memory_space=pltpu.VMEM), pl.BlockSpec(memory_space=pl.ANY)
    parts = pltpu.SemaphoreType.DMA((PARTS,))
    return pl.pallas_call(
        functools.partial(kernel, nx, ng),
        out_shape=pltpu.VMEM(pair.shape, low),
        in_specs=[where, where, vmem, where, where, vmem, where],
        out_specs=vmem,
        scratch_shapes=[
            pltpu.VMEM(pair.shape, low),
            pltpu.VMEM(pair_mask.shape, jnp.int32),
            pltpu.VMEM(input_weights.shape, low),
            pltpu.VMEM(out_gate_weight.shape, low),
            pltpu.VMEM(out_weight.shape, low),
            pltpu.VMEM((PARTS, channels, rows, LANES), low),
            pltpu.VMEM((PARTS, rows, channels, LANES), low),
            pltpu.VMEM((PARTS, hidden, rows, LANES), low),
            pltpu.VMEM((PARTS, hidden, rows, LANES), low),
            pltpu.VMEM((PARTS, long, LANES), low),
            pltpu.VMEM((PARTS, long, LANES), low),
            pltpu.VMEM((PARTS, long, LANES), low),
            pltpu.VMEM((2 * PARTS * LANES, long), low),
            pltpu.VMEM((PARTS, long, LANES), low),
            pltpu.VMEM((PARTS, hidden, rows, LANES), low),
            pltpu.VMEM((PARTS, channels, rows, LANES), low),
            pltpu.VMEM((PARTS, rows, channels, LANES), full),
            pltpu.VMEM((6 * channels, channels), low),
            pltpu.VMEM((2, channels, channels), full),
            pltpu.VMEM((channels * rows, LANES), full),
            pltpu.VMEM((channels * rows, LANES), full),
            pltpu.VMEM((PARTS, rows, LANES), full),
            pltpu.SemaphoreType.DMA((5,)),
            pltpu.SemaphoreType.DMA((5,)),
            parts,
            parts,
            parts,
            parts,
            parts,
            pltpu.SemaphoreType.DMA(()),
            pltpu.SemaphoreType.REGULAR,
        ],
        compiler_params=pltpu.CompilerParams(collective_id=0, has_side_effects=True),
    )(
        pair, pair_mask, input_gain[None], input_weights, out_gate_weight, hidden_gain[None], out_weight
    )


def solution(mesh):
    placed = (P("gz", "gx", "gy"), P("gx", "gy"), P(), P(), P(), P(), P())
    return jax.shard_map(
        functools.partial(shards, mesh),
        mesh=mesh,
        in_specs=placed,
        out_specs=P("gz", "gx", "gy"),
        check_vma=False,
    )
```

```python
import functools

import jax
import jax.numpy as jnp
from jax import lax
from jax.experimental import pallas as pl
from jax.experimental.pallas import tpu as pltpu
from jax.sharding import PartitionSpec as P

EPSILON = 1e-05
MESH = pl.DeviceIdType.MESH
LANES = 128
PARTS = 4


def statistics(values):
    average = jnp.mean(values, axis=0)
    centred = values - average
    return centred * lax.rsqrt(jnp.mean(jnp.square(centred), axis=0) + EPSILON)


def kernel(
    nx, ng,
    pair_in, mask_in, input_gain, input_weights_in, gate_weight_in, hidden_gain, out_weight_in,
    out,
    pair, mask, input_weights, gate_weight, out_weight,
    shared, ones, left, right, all_left, all_right, other_left, turned, passed, partner, kept,
    triangle, hidden, update, gate,
    weights, gains, rows_in, rows_out, rows_kept,
    loaded, send, got_shared, got_left, got_right, got_other, got_partner, got_hidden, got_out, planes,
):
    x, y, g = lax.axis_index("gx"), lax.axis_index("gy"), lax.axis_index("gz")
    chips = nx * ng
    reach = nx // 2
    depth = pair.shape[0]
    rows = pair.shape[1] // ng
    channels = gate_weight.shape[0]
    wide = PARTS * LANES
    tall = ng * rows

    def plane_at(far):
        return lax.rem(x + far + nx, nx)

    def owner_at(role, far):
        plane = plane_at(far - role * 2 * far)
        return plane, lax.rem(plane + nx - role, nx) * ng

    owners = {(role, far): owner_at(role, far) for role in range(2) for far in range(reach)}

    def aligned(at, size):
        return pl.ds(pl.multiple_of(at * size, size), size)

    barrier = pltpu.get_barrier_semaphore()

    @pl.loop(1, ng)
    def _(step):
        pl.semaphore_signal(
            barrier, inc=1, device_id=(x, y, lax.rem(g + step, ng)), device_id_type=MESH
        )

    line = [plane_at(far) for far in range(1 - reach, reach) if far]
    for plane in line:
        pl.semaphore_signal(barrier, inc=1, device_id=(plane, y, g), device_id_type=MESH)

    pl.semaphore_signal(barrier, inc=1, device_id=(x, 1 - y, g), device_id_type=MESH)

    loads = [
        pltpu.make_async_copy(there, here, loaded.at[k])
        for k, (there, here) in enumerate(
            (
                (pair_in, pair),
                (input_weights_in, input_weights),
                (gate_weight_in, gate_weight),
                (out_weight_in, out_weight),
                (mask_in, mask),
            )
        )
    ]
    for load in loads:
        load.start()
    gains[0] = jnp.broadcast_to(input_gain[...], (channels, channels)).T
    gains[1] = jnp.broadcast_to(hidden_gain[...], (channels, channels)).T
    for load in loads:
        load.wait()

    pl.semaphore_wait(barrier, ng + len(line))

    my_rows = aligned(g, rows)
    my_channels = aligned(g, depth)
    for q in range(PARTS):
        columns = pl.ds(q * LANES, LANES)

        @pl.loop(1, ng)
        def _(step):
            peer = lax.rem(g + step, ng)
            pltpu.make_async_remote_copy(
                src_ref=pair.at[:, aligned(peer, rows), columns],
                dst_ref=shared.at[q, my_channels],
                send_sem=send.at[0],
                recv_sem=got_shared.at[q],
                device_id=(x, y, peer),
                device_id_type=MESH,
            ).start()

        pltpu.make_async_copy(
            pair.at[:, my_rows, columns], shared.at[q, my_channels], got_shared.at[q]
        ).start()

    for plane in line:
        pl.semaphore_signal(planes, inc=1, device_id=(plane, y, g), device_id_type=MESH)

    for k in range(4):
        weights[k * channels : (k + 1) * channels] = (
            input_weights[k].astype(jnp.float32).T.astype(jnp.bfloat16)
        )
    weights[4 * channels : 5 * channels] = gate_weight[...].astype(jnp.float32).T.astype(jnp.bfloat16)
    weights[5 * channels :] = out_weight[...].astype(jnp.float32).T.astype(jnp.bfloat16)

    def to_owners(side, whole, got, q):
        def place(far):
            return aligned(far * ng + g, rows)

        def copies(turn, fars):
            column = lax.rem(g + turn, ng)
            for far in fars:
                for role in range(2):
                    plane, channel = owners[role, far]
                    pltpu.make_async_remote_copy(
                        src_ref=side.at[q, channel + column],
                        dst_ref=whole.at[q, role, place(far), :],
                        send_sem=send.at[1],
                        recv_sem=got.at[q],
                        device_id=(plane, y, column),
                        device_id_type=MESH,
                    ).start()

        copies(0, range(reach - 1, 0, -1))

        @pl.loop(1, ng)
        def _(turn):
            copies(turn, range(reach - 1, -1, -1))

        for role in range(2):
            pltpu.make_async_copy(
                side.at[q, owners[role, 0][1] + g], whole.at[q, role, place(0), :], got.at[q]
            ).start()

    for q in range(PARTS):
        pltpu.make_async_copy(shared.at[q], shared.at[q], got_shared.at[q]).wait()
        normed = statistics(shared[q].astype(jnp.float32))
        rows_in[...] = normed.reshape(channels * rows, LANES)
        rows_kept[q] = mask[my_rows, pl.ds(q * LANES, LANES)].astype(jnp.float32)

        @pl.loop(0, rows, unroll=8)
        def _(r):
            take = pl.ds(r, channels, stride=rows)
            one = (rows_in[take, :] * gains[0]).astype(jnp.bfloat16)
            ones[q, r] = one
            product = jnp.dot(weights[: 2 * channels], one, preferred_element_type=jnp.float32)
            rows_out[take, :] = (
                rows_kept[q, pl.ds(r, 1), :]
                * jax.nn.sigmoid(product[:channels])
                * product[channels:]
            )

        left[q] = rows_out[...].reshape(channels, rows, LANES).astype(jnp.bfloat16)
        if q == 0:
            pl.semaphore_wait(planes, len(line))
        to_owners(left, all_left, got_left, q)

    for q in range(PARTS):

        @pl.loop(0, rows, unroll=8)
        def _(r):
            product = jnp.dot(
                weights[2 * channels : 5 * channels], ones[q, r], preferred_element_type=jnp.float32
            )
            keep = rows_kept[q, pl.ds(r, 1), :]
            rows_out[pl.ds(r, channels, stride=rows), :] = (
                keep * jax.nn.sigmoid(product[:channels]) * product[channels : 2 * channels]
            )
            gate[q, r] = keep * jax.nn.sigmoid(product[2 * channels :])

        right[q] = rows_out[...].reshape(channels, rows, LANES).astype(jnp.bfloat16)
        to_owners(right, all_right, got_right, q)

    for q in range(PARTS):
        pltpu.make_async_copy(all_left.at[q], all_left.at[q], got_left.at[q]).wait()
        pltpu.make_async_remote_copy(
            src_ref=all_left.at[q],
            dst_ref=other_left.at[q],
            send_sem=send.at[2],
            recv_sem=got_other.at[q],
            device_id=(x, 1 - y, g),
            device_id_type=MESH,
        ).start()
        for role in range(2):
            turned[role, aligned(y * PARTS + q, LANES), :] = all_left[q, role].T
    for q in range(PARTS):
        pltpu.make_async_copy(other_left.at[q], other_left.at[q], got_other.at[q]).wait()
        for role in range(2):
            turned[role, aligned((1 - y) * PARTS + q, LANES), :] = other_left[q, role].T

    for q in range(PARTS):
        pltpu.make_async_copy(all_right.at[q], all_right.at[q], got_right.at[q]).wait()
        for role in range(2):
            side = 1 - 2 * role
            other = plane_at(side)

            def partial(plane):
                return jnp.dot(
                    turned[role, aligned(plane, tall), :],
                    all_right[q, role],
                    preferred_element_type=jnp.float32,
                )

            for far in range(reach):
                passed[q, role, far] = partial(plane_at(side * (far + 1))).astype(jnp.bfloat16)
            pltpu.make_async_remote_copy(
                src_ref=passed.at[q, role],
                dst_ref=partner.at[q, 1 - role],
                send_sem=send.at[5],
                recv_sem=got_partner.at[q],
                device_id=(other, y, g),
                device_id_type=MESH,
            ).start()
            for far in range(reach):
                kept[q, role, far] = partial(plane_at(-side * far))

    for q in range(PARTS):
        pltpu.make_async_copy(partner.at[q], partner.at[q], got_partner.at[q]).wait()

        for far in range(reach - 1, -1, -1):
            for role in range(2):
                triangle[q, role, far] = (
                    kept[q, role, far] + partner[q, role, far].astype(jnp.float32)
                ).astype(jnp.bfloat16)

            def copies(turn):
                column = lax.rem(g + turn, ng)
                for role in range(2):
                    pltpu.make_async_remote_copy(
                        src_ref=triangle.at[q, role, far, aligned(column, rows), :],
                        dst_ref=hidden.at[q, owners[role, 0][1] + g],
                        send_sem=send.at[3],
                        recv_sem=got_hidden.at[q],
                        device_id=(owners[1 - role, far][0], y, column),
                        device_id_type=MESH,
                    ).start()

            if far:
                copies(0)

            @pl.loop(1, ng, unroll=5)
            def _(turn):
                copies(turn)

        for role in range(2):
            pltpu.make_async_copy(
                triangle.at[q, role, 0, my_rows, :],
                hidden.at[q, owners[role, 0][1] + g],
                got_hidden.at[q],
            ).start()

    for q in range(PARTS):
        columns = pl.ds(q * LANES, LANES)
        pltpu.make_async_copy(hidden.at[q], hidden.at[q], got_hidden.at[q]).wait()
        normed = statistics(hidden[q].astype(jnp.float32))
        rows_in[...] = normed.reshape(channels * rows, LANES)

        @pl.loop(0, rows, unroll=8)
        def _(r):
            take = pl.ds(r, channels, stride=rows)
            one = (rows_in[take, :] * gains[1]).astype(jnp.bfloat16)
            projected = jnp.dot(weights[5 * channels :], one, preferred_element_type=jnp.float32)
            rows_out[take, :] = gate[q, r] * projected

        update[q] = rows_out[...].reshape(channels, rows, LANES).astype(jnp.bfloat16)

        @pl.loop(1, ng)
        def _(step):
            peer = lax.rem(g + step, ng)
            pltpu.make_async_remote_copy(
                src_ref=update.at[q, aligned(peer, depth)],
                dst_ref=out.at[:, my_rows, columns],
                send_sem=send.at[4],
                recv_sem=got_out,
                device_id=(x, y, peer),
                device_id_type=MESH,
            ).start()

        pltpu.make_async_copy(update.at[q, my_channels], out.at[:, my_rows, columns], got_out).start()

    pltpu.make_async_copy(out, out, got_out).wait()
    for q in range(PARTS):
        few = shared.at[q, pl.ds(0, (ng - 1) * depth)]
        pltpu.make_async_copy(few, few, send.at[0]).wait()
        for side in (left, right):
            most = side.at[q, pl.ds(0, chips - 2)]
            pltpu.make_async_copy(most, most, send.at[1]).wait()
        pltpu.make_async_copy(other_left.at[q], other_left.at[q], send.at[2]).wait()
        pltpu.make_async_copy(passed.at[q], passed.at[q], send.at[5]).wait()
        most = hidden.at[q, pl.ds(0, chips - 2)]
        pltpu.make_async_copy(most, most, send.at[3]).wait()
        few = update.at[q, pl.ds(0, (ng - 1) * depth)]
        pltpu.make_async_copy(few, few, send.at[4]).wait()


def shards(mesh, pair, pair_mask, input_gain, input_weights, out_gate_weight, hidden_gain, out_weight):
    nx, ng = mesh.shape["gx"], mesh.shape["gz"]
    channels, hidden = input_weights.shape[1:]
    tall, reach = pair.shape[1], nx // 2
    rows, near = tall // ng, tall * reach
    low, full = jnp.bfloat16, jnp.float32
    vmem, where = pl.BlockSpec(memory_space=pltpu.VMEM), pl.BlockSpec(memory_space=pl.ANY)
    parts = pltpu.SemaphoreType.DMA((PARTS,))
    return pl.pallas_call(
        functools.partial(kernel, nx, ng),
        out_shape=pltpu.VMEM(pair.shape, low),
        in_specs=[where, where, vmem, where, where, vmem, where],
        out_specs=vmem,
        scratch_shapes=[
            pltpu.VMEM(pair.shape, low),
            pltpu.VMEM(pair_mask.shape, jnp.int32),
            pltpu.VMEM(input_weights.shape, low),
            pltpu.VMEM(out_gate_weight.shape, low),
            pltpu.VMEM(out_weight.shape, low),
            pltpu.VMEM((PARTS, channels, rows, LANES), low),
            pltpu.VMEM((PARTS, rows, channels, LANES), low),
            pltpu.VMEM((PARTS, hidden, rows, LANES), low),
            pltpu.VMEM((PARTS, hidden, rows, LANES), low),
            pltpu.VMEM((PARTS, 2, near, LANES), low),
            pltpu.VMEM((PARTS, 2, near, LANES), low),
            pltpu.VMEM((PARTS, 2, near, LANES), low),
            pltpu.VMEM((2, 2 * PARTS * LANES, near), low),
            pltpu.VMEM((PARTS, 2, reach, tall, LANES), low),
            pltpu.VMEM((PARTS, 2, reach, tall, LANES), low),
            pltpu.VMEM((PARTS, 2, reach, tall, LANES), full),
            pltpu.VMEM((PARTS, 2, reach, tall, LANES), low),
            pltpu.VMEM((PARTS, hidden, rows, LANES), low),
            pltpu.VMEM((PARTS, channels, rows, LANES), low),
            pltpu.VMEM((PARTS, rows, channels, LANES), full),
            pltpu.VMEM((6 * channels, channels), low),
            pltpu.VMEM((2, channels, channels), full),
            pltpu.VMEM((channels * rows, LANES), full),
            pltpu.VMEM((channels * rows, LANES), full),
            pltpu.VMEM((PARTS, rows, LANES), full),
            pltpu.SemaphoreType.DMA((5,)),
            pltpu.SemaphoreType.DMA((6,)),
            parts,
            parts,
            parts,
            parts,
            parts,
            parts,
            pltpu.SemaphoreType.DMA(()),
            pltpu.SemaphoreType.REGULAR,
        ],
        compiler_params=pltpu.CompilerParams(collective_id=0, has_side_effects=True),
    )(
        pair, pair_mask, input_gain[None], input_weights, out_gate_weight, hidden_gain[None], out_weight
    )


def solution(mesh):
    placed = (P("gz", "gx", "gy"), P("gx", "gy"), P(), P(), P(), P(), P())
    return jax.shard_map(
        functools.partial(shards, mesh),
        mesh=mesh,
        in_specs=placed,
        out_specs=P("gz", "gx", "gy"),
        check_vma=False,
    )
```

```python
import functools

import jax
import jax.numpy as jnp
from jax import lax
from jax.experimental import pallas as pl
from jax.experimental.pallas import tpu as pltpu
from jax.sharding import PartitionSpec as P

EPSILON = 1e-05
MESH = pl.DeviceIdType.MESH
LANES = 128
PARTS = 4


def statistics(values):
    average = jnp.mean(values, axis=0)
    centred = values - average
    return centred * lax.rsqrt(jnp.mean(jnp.square(centred), axis=0) + EPSILON)


def kernel(
    nx, ng,
    pair_in, mask_in, input_gain, input_weights_in, gate_weight_in, hidden_gain, out_weight_in,
    out,
    pair, mask, input_weights, gate_weight, out_weight,
    shared, ones, left, right, all_left, all_right, other_left, turned, passed, partner, kept,
    triangle, hidden, update, gate,
    weights, gains, rows_in, rows_out, rows_kept,
    loaded, send, got_shared, got_left, got_right, got_other, got_partner, got_hidden, got_out, planes,
):
    x, y, g = lax.axis_index("gx"), lax.axis_index("gy"), lax.axis_index("gz")
    chips = nx * ng
    reach = nx // 2
    depth = pair.shape[0]
    rows = pair.shape[1] // ng
    channels = gate_weight.shape[0]
    wide = PARTS * LANES
    tall = ng * rows

    def plane_at(far):
        return lax.rem(x + far + nx, nx)

    def owner_at(role, far):
        plane = plane_at(far - role * 2 * far)
        return plane, lax.rem(plane + nx - role, nx) * ng

    owners = {(role, far): owner_at(role, far) for role in range(2) for far in range(reach)}

    def aligned(at, size):
        return pl.ds(pl.multiple_of(at * size, size), size)

    def far_first():
        side = round(ng**0.5)
        apart = [(dy, dx) for dy in range(side) for dx in range(side) if dy or dx]

        def hops(d):
            return min(d, side - d)

        apart.sort(key=lambda d: -(hops(d[0]) + hops(d[1])))
        return [
            lax.rem(g // side + dy, side) * side + lax.rem(lax.rem(g, side) + dx, side)
            for dy, dx in apart
        ]

    peers = far_first()
    barrier = pltpu.get_barrier_semaphore()

    for peer in peers:
        pl.semaphore_signal(barrier, inc=1, device_id=(x, y, peer), device_id_type=MESH)

    line = [plane_at(far) for far in range(1 - reach, reach) if far]
    for plane in line:
        pl.semaphore_signal(barrier, inc=1, device_id=(plane, y, g), device_id_type=MESH)

    pl.semaphore_signal(barrier, inc=1, device_id=(x, 1 - y, g), device_id_type=MESH)

    loads = [
        pltpu.make_async_copy(there, here, loaded.at[k])
        for k, (there, here) in enumerate(
            (
                (pair_in, pair),
                (input_weights_in, input_weights),
                (gate_weight_in, gate_weight),
                (out_weight_in, out_weight),
                (mask_in, mask),
            )
        )
    ]
    for load in loads:
        load.start()
    gains[0] = jnp.broadcast_to(input_gain[...], (channels, channels)).T
    gains[1] = jnp.broadcast_to(hidden_gain[...], (channels, channels)).T
    for load in loads:
        load.wait()

    pl.semaphore_wait(barrier, ng + len(line))

    my_rows = aligned(g, rows)
    my_channels = aligned(g, depth)
    for q in range(PARTS):
        columns = pl.ds(q * LANES, LANES)

        for peer in peers:
            pltpu.make_async_remote_copy(
                src_ref=pair.at[:, aligned(peer, rows), columns],
                dst_ref=shared.at[q, my_channels],
                send_sem=send.at[0],
                recv_sem=got_shared.at[q],
                device_id=(x, y, peer),
                device_id_type=MESH,
            ).start()

        pltpu.make_async_copy(
            pair.at[:, my_rows, columns], shared.at[q, my_channels], got_shared.at[q]
        ).start()

    for plane in line:
        pl.semaphore_signal(planes, inc=1, device_id=(plane, y, g), device_id_type=MESH)

    for k in range(4):
        weights[k * channels : (k + 1) * channels] = (
            input_weights[k].astype(jnp.float32).T.astype(jnp.bfloat16)
        )
    weights[4 * channels : 5 * channels] = gate_weight[...].astype(jnp.float32).T.astype(jnp.bfloat16)
    weights[5 * channels :] = out_weight[...].astype(jnp.float32).T.astype(jnp.bfloat16)

    def to_owners(side, whole, got, q):
        def place(far):
            return aligned(far * ng + g, rows)

        def copies(turn, fars):
            column = lax.rem(g + turn, ng)
            for far in fars:
                for role in range(2):
                    plane, channel = owners[role, far]
                    pltpu.make_async_remote_copy(
                        src_ref=side.at[q, channel + column],
                        dst_ref=whole.at[q, role, place(far), :],
                        send_sem=send.at[1],
                        recv_sem=got.at[q],
                        device_id=(plane, y, column),
                        device_id_type=MESH,
                    ).start()

        copies(0, range(reach - 1, 0, -1))

        @pl.loop(1, ng)
        def _(turn):
            copies(turn, range(reach - 1, -1, -1))

        for role in range(2):
            pltpu.make_async_copy(
                side.at[q, owners[role, 0][1] + g], whole.at[q, role, place(0), :], got.at[q]
            ).start()

    for q in range(PARTS):
        pltpu.make_async_copy(shared.at[q], shared.at[q], got_shared.at[q]).wait()
        normed = statistics(shared[q].astype(jnp.float32))
        rows_in[...] = normed.reshape(channels * rows, LANES)
        rows_kept[q] = mask[my_rows, pl.ds(q * LANES, LANES)].astype(jnp.float32)

        @pl.loop(0, rows, unroll=8)
        def _(r):
            take = pl.ds(r, channels, stride=rows)
            one = (rows_in[take, :] * gains[0]).astype(jnp.bfloat16)
            ones[q, r] = one
            product = jnp.dot(weights[: 2 * channels], one, preferred_element_type=jnp.float32)
            rows_out[take, :] = (
                rows_kept[q, pl.ds(r, 1), :]
                * jax.nn.sigmoid(product[:channels])
                * product[channels:]
            )

        left[q] = rows_out[...].reshape(channels, rows, LANES).astype(jnp.bfloat16)
        if q == 0:
            pl.semaphore_wait(planes, len(line))
        to_owners(left, all_left, got_left, q)

    for q in range(PARTS):

        @pl.loop(0, rows, unroll=8)
        def _(r):
            product = jnp.dot(
                weights[2 * channels : 5 * channels], ones[q, r], preferred_element_type=jnp.float32
            )
            keep = rows_kept[q, pl.ds(r, 1), :]
            rows_out[pl.ds(r, channels, stride=rows), :] = (
                keep * jax.nn.sigmoid(product[:channels]) * product[channels : 2 * channels]
            )
            gate[q, r] = keep * jax.nn.sigmoid(product[2 * channels :])

        right[q] = rows_out[...].reshape(channels, rows, LANES).astype(jnp.bfloat16)
        to_owners(right, all_right, got_right, q)

    for q in range(PARTS):
        pltpu.make_async_copy(all_left.at[q], all_left.at[q], got_left.at[q]).wait()
        pltpu.make_async_remote_copy(
            src_ref=all_left.at[q],
            dst_ref=other_left.at[q],
            send_sem=send.at[2],
            recv_sem=got_other.at[q],
            device_id=(x, 1 - y, g),
            device_id_type=MESH,
        ).start()
        for role in range(2):
            turned[role, aligned(y * PARTS + q, LANES), :] = all_left[q, role].T
    for q in range(PARTS):
        pltpu.make_async_copy(other_left.at[q], other_left.at[q], got_other.at[q]).wait()
        for role in range(2):
            turned[role, aligned((1 - y) * PARTS + q, LANES), :] = other_left[q, role].T

    def swap(q):
        pltpu.make_async_copy(all_right.at[q], all_right.at[q], got_right.at[q]).wait()
        for role in range(2):
            side = 1 - 2 * role
            other = plane_at(side)

            def partial(plane):
                return jnp.dot(
                    turned[role, aligned(plane, tall), :],
                    all_right[q, role],
                    preferred_element_type=jnp.float32,
                )

            for far in range(reach):
                passed[q, role, far] = partial(plane_at(side * (far + 1))).astype(jnp.bfloat16)
            pltpu.make_async_remote_copy(
                src_ref=passed.at[q, role],
                dst_ref=partner.at[q, 1 - role],
                send_sem=send.at[5],
                recv_sem=got_partner.at[q],
                device_id=(other, y, g),
                device_id_type=MESH,
            ).start()
            for far in range(reach):
                kept[q, role, far] = partial(plane_at(-side * far))

    def finish(q):
        pltpu.make_async_copy(partner.at[q], partner.at[q], got_partner.at[q]).wait()

        for far in range(reach - 1, -1, -1):
            for role in range(2):
                triangle[q, role, far] = (
                    kept[q, role, far] + partner[q, role, far].astype(jnp.float32)
                ).astype(jnp.bfloat16)

            def copies(turn):
                column = lax.rem(g + turn, ng)
                for role in range(2):
                    pltpu.make_async_remote_copy(
                        src_ref=triangle.at[q, role, far, aligned(column, rows), :],
                        dst_ref=hidden.at[q, owners[role, 0][1] + g],
                        send_sem=send.at[3],
                        recv_sem=got_hidden.at[q],
                        device_id=(owners[1 - role, far][0], y, column),
                        device_id_type=MESH,
                    ).start()

            if far:
                copies(0)

            @pl.loop(1, ng, unroll=5)
            def _(turn):
                copies(turn)

        for role in range(2):
            pltpu.make_async_copy(
                triangle.at[q, role, 0, my_rows, :],
                hidden.at[q, owners[role, 0][1] + g],
                got_hidden.at[q],
            ).start()

    for q in range(PARTS):
        swap(q)
        if q > 1:
            finish(q - 2)
    for q in range(PARTS - 2, PARTS):
        finish(q)

    for q in range(PARTS):
        columns = pl.ds(q * LANES, LANES)
        pltpu.make_async_copy(hidden.at[q], hidden.at[q], got_hidden.at[q]).wait()
        normed = statistics(hidden[q].astype(jnp.float32))
        rows_in[...] = normed.reshape(channels * rows, LANES)

        @pl.loop(0, rows, unroll=8)
        def _(r):
            take = pl.ds(r, channels, stride=rows)
            one = (rows_in[take, :] * gains[1]).astype(jnp.bfloat16)
            projected = jnp.dot(weights[5 * channels :], one, preferred_element_type=jnp.float32)
            rows_out[take, :] = gate[q, r] * projected

        update[q] = rows_out[...].reshape(channels, rows, LANES).astype(jnp.bfloat16)

        for peer in peers:
            pltpu.make_async_remote_copy(
                src_ref=update.at[q, aligned(peer, depth)],
                dst_ref=out.at[:, my_rows, columns],
                send_sem=send.at[4],
                recv_sem=got_out,
                device_id=(x, y, peer),
                device_id_type=MESH,
            ).start()

        pltpu.make_async_copy(update.at[q, my_channels], out.at[:, my_rows, columns], got_out).start()

    pltpu.make_async_copy(out, out, got_out).wait()
    for q in range(PARTS):
        few = shared.at[q, pl.ds(0, (ng - 1) * depth)]
        pltpu.make_async_copy(few, few, send.at[0]).wait()
        for side in (left, right):
            most = side.at[q, pl.ds(0, chips - 2)]
            pltpu.make_async_copy(most, most, send.at[1]).wait()
        pltpu.make_async_copy(other_left.at[q], other_left.at[q], send.at[2]).wait()
        pltpu.make_async_copy(passed.at[q], passed.at[q], send.at[5]).wait()
        most = hidden.at[q, pl.ds(0, chips - 2)]
        pltpu.make_async_copy(most, most, send.at[3]).wait()
        few = update.at[q, pl.ds(0, (ng - 1) * depth)]
        pltpu.make_async_copy(few, few, send.at[4]).wait()


def shards(mesh, pair, pair_mask, input_gain, input_weights, out_gate_weight, hidden_gain, out_weight):
    nx, ng = mesh.shape["gx"], mesh.shape["gz"]
    channels, hidden = input_weights.shape[1:]
    tall, reach = pair.shape[1], nx // 2
    rows, near = tall // ng, tall * reach
    low, full = jnp.bfloat16, jnp.float32
    vmem, where = pl.BlockSpec(memory_space=pltpu.VMEM), pl.BlockSpec(memory_space=pl.ANY)
    parts = pltpu.SemaphoreType.DMA((PARTS,))
    return pl.pallas_call(
        functools.partial(kernel, nx, ng),
        out_shape=pltpu.VMEM(pair.shape, low),
        in_specs=[where, where, vmem, where, where, vmem, where],
        out_specs=vmem,
        scratch_shapes=[
            pltpu.VMEM(pair.shape, low),
            pltpu.VMEM(pair_mask.shape, jnp.int32),
            pltpu.VMEM(input_weights.shape, low),
            pltpu.VMEM(out_gate_weight.shape, low),
            pltpu.VMEM(out_weight.shape, low),
            pltpu.VMEM((PARTS, channels, rows, LANES), low),
            pltpu.VMEM((PARTS, rows, channels, LANES), low),
            pltpu.VMEM((PARTS, hidden, rows, LANES), low),
            pltpu.VMEM((PARTS, hidden, rows, LANES), low),
            pltpu.VMEM((PARTS, 2, near, LANES), low),
            pltpu.VMEM((PARTS, 2, near, LANES), low),
            pltpu.VMEM((PARTS, 2, near, LANES), low),
            pltpu.VMEM((2, 2 * PARTS * LANES, near), low),
            pltpu.VMEM((PARTS, 2, reach, tall, LANES), low),
            pltpu.VMEM((PARTS, 2, reach, tall, LANES), low),
            pltpu.VMEM((PARTS, 2, reach, tall, LANES), full),
            pltpu.VMEM((PARTS, 2, reach, tall, LANES), low),
            pltpu.VMEM((PARTS, hidden, rows, LANES), low),
            pltpu.VMEM((PARTS, channels, rows, LANES), low),
            pltpu.VMEM((PARTS, rows, channels, LANES), full),
            pltpu.VMEM((6 * channels, channels), low),
            pltpu.VMEM((2, channels, channels), full),
            pltpu.VMEM((channels * rows, LANES), full),
            pltpu.VMEM((channels * rows, LANES), full),
            pltpu.VMEM((PARTS, rows, LANES), full),
            pltpu.SemaphoreType.DMA((5,)),
            pltpu.SemaphoreType.DMA((6,)),
            parts,
            parts,
            parts,
            parts,
            parts,
            parts,
            pltpu.SemaphoreType.DMA(()),
            pltpu.SemaphoreType.REGULAR,
        ],
        compiler_params=pltpu.CompilerParams(collective_id=0, has_side_effects=True),
    )(
        pair, pair_mask, input_gain[None], input_weights, out_gate_weight, hidden_gain[None], out_weight
    )


def solution(mesh):
    placed = (P("gz", "gx", "gy"), P("gx", "gy"), P(), P(), P(), P(), P())
    return jax.shard_map(
        functools.partial(shards, mesh),
        mesh=mesh,
        in_specs=placed,
        out_specs=P("gz", "gx", "gy"),
        check_vma=False,
    )
```

```python
import functools

import jax
import jax.numpy as jnp
from jax import lax
from jax.experimental import pallas as pl
from jax.experimental.pallas import tpu as pltpu
from jax.sharding import PartitionSpec as P

EPSILON = 1e-05
MESH = pl.DeviceIdType.MESH
LANES = 128
PARTS = 4


def statistics(values):
    average = jnp.mean(values, axis=0)
    centred = values - average
    return centred * lax.rsqrt(jnp.mean(jnp.square(centred), axis=0) + EPSILON)


def kernel(
    nx, ng,
    pair_in, mask_in, input_gain, input_weights_in, gate_weight_in, hidden_gain, out_weight_in,
    out,
    pair, mask, input_weights, gate_weight, out_weight,
    shared, ones, left, right, all_left, all_right, other_left, turned, passed, partner, kept,
    triangle, hidden, update, gate,
    weights, gains, rows_in, rows_out, rows_kept,
    loaded, send, got_shared, got_left, got_right, got_other, got_partner, got_hidden, got_out, planes,
):
    x, y, g = lax.axis_index("gx"), lax.axis_index("gy"), lax.axis_index("gz")
    chips = nx * ng
    reach = nx // 2
    depth = pair.shape[0]
    rows = pair.shape[1] // ng
    channels = gate_weight.shape[0]
    wide = PARTS * LANES
    tall = ng * rows

    def plane_at(far):
        return lax.rem(x + far + nx, nx)

    def owner_at(role, far):
        plane = plane_at(far - role * 2 * far)
        return plane, lax.rem(plane + nx - role, nx) * ng

    owners = {(role, far): owner_at(role, far) for role in range(2) for far in range(reach)}

    def aligned(at, size):
        return pl.ds(pl.multiple_of(at * size, size), size)

    def far_first():
        side = round(ng**0.5)
        apart = [(dy, dx) for dy in range(side) for dx in range(side) if dy or dx]

        def hops(d):
            return min(d, side - d)

        apart.sort(key=lambda d: -(hops(d[0]) + hops(d[1])))
        return [
            lax.rem(g // side + dy, side) * side + lax.rem(lax.rem(g, side) + dx, side)
            for dy, dx in apart
        ]

    peers = far_first()
    barrier = pltpu.get_barrier_semaphore()

    for peer in peers:
        pl.semaphore_signal(barrier, inc=1, device_id=(x, y, peer), device_id_type=MESH)

    line = [plane_at(far) for far in range(1 - reach, reach) if far]
    for plane in line:
        pl.semaphore_signal(barrier, inc=1, device_id=(plane, y, g), device_id_type=MESH)

    pl.semaphore_signal(barrier, inc=1, device_id=(x, 1 - y, g), device_id_type=MESH)

    loads = [
        pltpu.make_async_copy(there, here, loaded.at[k])
        for k, (there, here) in enumerate(
            (
                (pair_in, pair),
                (input_weights_in, input_weights),
                (gate_weight_in, gate_weight),
                (out_weight_in, out_weight),
                (mask_in, mask),
            )
        )
    ]
    for load in loads:
        load.start()
    gains[0] = jnp.broadcast_to(input_gain[...], (channels, channels)).T
    gains[1] = jnp.broadcast_to(hidden_gain[...], (channels, channels)).T
    for load in loads:
        load.wait()

    pl.semaphore_wait(barrier, ng + len(line))

    my_rows = aligned(g, rows)
    my_channels = aligned(g, depth)
    for q in range(PARTS):
        columns = pl.ds(q * LANES, LANES)

        for peer in peers:
            pltpu.make_async_remote_copy(
                src_ref=pair.at[:, aligned(peer, rows), columns],
                dst_ref=shared.at[q, my_channels],
                send_sem=send.at[0],
                recv_sem=got_shared.at[q],
                device_id=(x, y, peer),
                device_id_type=MESH,
            ).start()

        pltpu.make_async_copy(
            pair.at[:, my_rows, columns], shared.at[q, my_channels], got_shared.at[q]
        ).start()

    for plane in line:
        pl.semaphore_signal(planes, inc=1, device_id=(plane, y, g), device_id_type=MESH)

    for k in range(4):
        weights[k * channels : (k + 1) * channels] = (
            input_weights[k].astype(jnp.float32).T.astype(jnp.bfloat16)
        )
    weights[4 * channels : 5 * channels] = gate_weight[...].astype(jnp.float32).T.astype(jnp.bfloat16)
    weights[5 * channels :] = out_weight[...].astype(jnp.float32).T.astype(jnp.bfloat16)

    def to_owners(side, whole, got, q):
        def place(far):
            return aligned(far * ng + g, rows)

        def copies(turn, fars):
            column = lax.rem(g + turn, ng)
            for far in fars:
                for role in range(2):
                    plane, channel = owners[role, far]
                    pltpu.make_async_remote_copy(
                        src_ref=side.at[q, channel + column],
                        dst_ref=whole.at[q, role, place(far), :],
                        send_sem=send.at[1],
                        recv_sem=got.at[q],
                        device_id=(plane, y, column),
                        device_id_type=MESH,
                    ).start()

        copies(0, range(1, reach))

        @pl.loop(1, ng)
        def _(turn):
            copies(turn, range(reach))

        for role in range(2):
            pltpu.make_async_copy(
                side.at[q, owners[role, 0][1] + g], whole.at[q, role, place(0), :], got.at[q]
            ).start()

    for q in range(PARTS):
        pltpu.make_async_copy(shared.at[q], shared.at[q], got_shared.at[q]).wait()
        normed = statistics(shared[q].astype(jnp.float32))
        rows_in[...] = normed.reshape(channels * rows, LANES)
        rows_kept[q] = mask[my_rows, pl.ds(q * LANES, LANES)].astype(jnp.float32)

        @pl.loop(0, rows, unroll=8)
        def _(r):
            take = pl.ds(r, channels, stride=rows)
            one = (rows_in[take, :] * gains[0]).astype(jnp.bfloat16)
            ones[q, r] = one
            product = jnp.dot(weights[: 2 * channels], one, preferred_element_type=jnp.float32)
            rows_out[take, :] = (
                rows_kept[q, pl.ds(r, 1), :]
                * jax.nn.sigmoid(product[:channels])
                * product[channels:]
            )

        left[q] = rows_out[...].reshape(channels, rows, LANES).astype(jnp.bfloat16)
        if q == 0:
            pl.semaphore_wait(planes, len(line))
        to_owners(left, all_left, got_left, q)

    for q in range(PARTS):

        @pl.loop(0, rows, unroll=8)
        def _(r):
            product = jnp.dot(
                weights[2 * channels : 5 * channels], ones[q, r], preferred_element_type=jnp.float32
            )
            keep = rows_kept[q, pl.ds(r, 1), :]
            rows_out[pl.ds(r, channels, stride=rows), :] = (
                keep * jax.nn.sigmoid(product[:channels]) * product[channels : 2 * channels]
            )
            gate[q, r] = keep * jax.nn.sigmoid(product[2 * channels :])

        right[q] = rows_out[...].reshape(channels, rows, LANES).astype(jnp.bfloat16)
        to_owners(right, all_right, got_right, q)

    for q in range(PARTS):
        pltpu.make_async_copy(all_left.at[q], all_left.at[q], got_left.at[q]).wait()
        pltpu.make_async_remote_copy(
            src_ref=all_left.at[q],
            dst_ref=other_left.at[q],
            send_sem=send.at[2],
            recv_sem=got_other.at[q],
            device_id=(x, 1 - y, g),
            device_id_type=MESH,
        ).start()
        for role in range(2):
            turned[role, aligned(y * PARTS + q, LANES), :] = all_left[q, role].T
    for q in range(PARTS):
        pltpu.make_async_copy(other_left.at[q], other_left.at[q], got_other.at[q]).wait()
        for role in range(2):
            turned[role, aligned((1 - y) * PARTS + q, LANES), :] = other_left[q, role].T

    def swap(q):
        pltpu.make_async_copy(all_right.at[q], all_right.at[q], got_right.at[q]).wait()
        for role in range(2):
            side = 1 - 2 * role
            other = plane_at(side)

            def partial(plane):
                return jnp.dot(
                    turned[role, aligned(plane, tall), :],
                    all_right[q, role],
                    preferred_element_type=jnp.float32,
                )

            for far in range(reach):
                passed[q, role, far] = partial(plane_at(side * (far + 1))).astype(jnp.bfloat16)
            pltpu.make_async_remote_copy(
                src_ref=passed.at[q, role],
                dst_ref=partner.at[q, 1 - role],
                send_sem=send.at[5],
                recv_sem=got_partner.at[q],
                device_id=(other, y, g),
                device_id_type=MESH,
            ).start()
            for far in range(reach):
                kept[q, role, far] = partial(plane_at(-side * far))

    def finish(q):
        pltpu.make_async_copy(partner.at[q], partner.at[q], got_partner.at[q]).wait()

        for far in range(reach - 1, -1, -1):
            for role in range(2):
                triangle[q, role, far] = (
                    kept[q, role, far] + partner[q, role, far].astype(jnp.float32)
                ).astype(jnp.bfloat16)

            def copies(turn):
                column = lax.rem(g + turn, ng)
                for role in range(2):
                    pltpu.make_async_remote_copy(
                        src_ref=triangle.at[q, role, far, aligned(column, rows), :],
                        dst_ref=hidden.at[q, owners[role, 0][1] + g],
                        send_sem=send.at[3],
                        recv_sem=got_hidden.at[q],
                        device_id=(owners[1 - role, far][0], y, column),
                        device_id_type=MESH,
                    ).start()

            if far:
                copies(0)

            @pl.loop(1, ng, unroll=5)
            def _(turn):
                copies(turn)

        for role in range(2):
            pltpu.make_async_copy(
                triangle.at[q, role, 0, my_rows, :],
                hidden.at[q, owners[role, 0][1] + g],
                got_hidden.at[q],
            ).start()

    for q in range(PARTS):
        swap(q)
        if q > 1:
            finish(q - 2)
    for q in range(PARTS - 2, PARTS):
        finish(q)

    for q in range(PARTS):
        columns = pl.ds(q * LANES, LANES)
        pltpu.make_async_copy(hidden.at[q], hidden.at[q], got_hidden.at[q]).wait()
        normed = statistics(hidden[q].astype(jnp.float32))
        rows_in[...] = normed.reshape(channels * rows, LANES)

        @pl.loop(0, rows, unroll=8)
        def _(r):
            take = pl.ds(r, channels, stride=rows)
            one = (rows_in[take, :] * gains[1]).astype(jnp.bfloat16)
            projected = jnp.dot(weights[5 * channels :], one, preferred_element_type=jnp.float32)
            rows_out[take, :] = gate[q, r] * projected

        update[q] = rows_out[...].reshape(channels, rows, LANES).astype(jnp.bfloat16)

        for peer in peers:
            pltpu.make_async_remote_copy(
                src_ref=update.at[q, aligned(peer, depth)],
                dst_ref=out.at[:, my_rows, columns],
                send_sem=send.at[4],
                recv_sem=got_out,
                device_id=(x, y, peer),
                device_id_type=MESH,
            ).start()

        pltpu.make_async_copy(update.at[q, my_channels], out.at[:, my_rows, columns], got_out).start()

    pltpu.make_async_copy(out, out, got_out).wait()
    for q in range(PARTS):
        few = shared.at[q, pl.ds(0, (ng - 1) * depth)]
        pltpu.make_async_copy(few, few, send.at[0]).wait()
        for side in (left, right):
            most = side.at[q, pl.ds(0, chips - 2)]
            pltpu.make_async_copy(most, most, send.at[1]).wait()
        pltpu.make_async_copy(other_left.at[q], other_left.at[q], send.at[2]).wait()
        pltpu.make_async_copy(passed.at[q], passed.at[q], send.at[5]).wait()
        most = hidden.at[q, pl.ds(0, chips - 2)]
        pltpu.make_async_copy(most, most, send.at[3]).wait()
        few = update.at[q, pl.ds(0, (ng - 1) * depth)]
        pltpu.make_async_copy(few, few, send.at[4]).wait()


def shards(mesh, pair, pair_mask, input_gain, input_weights, out_gate_weight, hidden_gain, out_weight):
    nx, ng = mesh.shape["gx"], mesh.shape["gz"]
    channels, hidden = input_weights.shape[1:]
    tall, reach = pair.shape[1], nx // 2
    rows, near = tall // ng, tall * reach
    low, full = jnp.bfloat16, jnp.float32
    vmem, where = pl.BlockSpec(memory_space=pltpu.VMEM), pl.BlockSpec(memory_space=pl.ANY)
    parts = pltpu.SemaphoreType.DMA((PARTS,))
    return pl.pallas_call(
        functools.partial(kernel, nx, ng),
        out_shape=pltpu.VMEM(pair.shape, low),
        in_specs=[where, where, vmem, where, where, vmem, where],
        out_specs=vmem,
        scratch_shapes=[
            pltpu.VMEM(pair.shape, low),
            pltpu.VMEM(pair_mask.shape, jnp.int32),
            pltpu.VMEM(input_weights.shape, low),
            pltpu.VMEM(out_gate_weight.shape, low),
            pltpu.VMEM(out_weight.shape, low),
            pltpu.VMEM((PARTS, channels, rows, LANES), low),
            pltpu.VMEM((PARTS, rows, channels, LANES), low),
            pltpu.VMEM((PARTS, hidden, rows, LANES), low),
            pltpu.VMEM((PARTS, hidden, rows, LANES), low),
            pltpu.VMEM((PARTS, 2, near, LANES), low),
            pltpu.VMEM((PARTS, 2, near, LANES), low),
            pltpu.VMEM((PARTS, 2, near, LANES), low),
            pltpu.VMEM((2, 2 * PARTS * LANES, near), low),
            pltpu.VMEM((PARTS, 2, reach, tall, LANES), low),
            pltpu.VMEM((PARTS, 2, reach, tall, LANES), low),
            pltpu.VMEM((PARTS, 2, reach, tall, LANES), full),
            pltpu.VMEM((PARTS, 2, reach, tall, LANES), low),
            pltpu.VMEM((PARTS, hidden, rows, LANES), low),
            pltpu.VMEM((PARTS, channels, rows, LANES), low),
            pltpu.VMEM((PARTS, rows, channels, LANES), full),
            pltpu.VMEM((6 * channels, channels), low),
            pltpu.VMEM((2, channels, channels), full),
            pltpu.VMEM((channels * rows, LANES), full),
            pltpu.VMEM((channels * rows, LANES), full),
            pltpu.VMEM((PARTS, rows, LANES), full),
            pltpu.SemaphoreType.DMA((5,)),
            pltpu.SemaphoreType.DMA((6,)),
            parts,
            parts,
            parts,
            parts,
            parts,
            parts,
            pltpu.SemaphoreType.DMA(()),
            pltpu.SemaphoreType.REGULAR,
        ],
        compiler_params=pltpu.CompilerParams(collective_id=0, has_side_effects=True),
    )(
        pair, pair_mask, input_gain[None], input_weights, out_gate_weight, hidden_gain[None], out_weight
    )


def solution(mesh):
    placed = (P("gz", "gx", "gy"), P("gx", "gy"), P(), P(), P(), P(), P())
    return jax.shard_map(
        functools.partial(shards, mesh),
        mesh=mesh,
        in_specs=placed,
        out_specs=P("gz", "gx", "gy"),
        check_vma=False,
    )
```
